32 devices in a mesh: dp: 4 (over z), expert: 4 (over x, core), shard: 2 (over y).
Axes of the slice: x: 2, y: 2, z: 4, core: 2. Of those that a mesh axis runs over, the one named last changes fastest.
Arguments:
- tokens: bfloat16 [4, 1024, 2048], P('dp', ('expert', 'shard')), may hold values from -6 to 6
- norm_gains: float32 [2, 2048], replicated, may hold values from 0.5 to 1.5
- routers: float32 [2, 2048, 4], replicated, may hold values from -0.09375 to 0.09375
- kv_weight: bfloat16 [2048, 4096], P(('dp', 'expert', 'shard')), may hold values from -0.125 to 0.125
- query_weight: bfloat16 [4, 2048, 2048], P('expert', ('dp', 'shard')), may hold values from -0.125 to 0.125
- output_weight: bfloat16 [4, 2048, 2048], P('expert', ('dp', 'shard')), may hold values from -1 to 1
- inner_weight: bfloat16 [4, 2048, 11264], P('expert', ('dp', 'shard')), may hold values from -0.125 to 0.125
- outer_weight: bfloat16 [4, 5632, 2048], P('expert', ('dp', 'shard')), may hold values from -0.078125 to 0.078125
- route_attn: int32 [4, 1024, 2], P('dp', ('expert', 'shard')), may hold values from 0 to 3, all different within a row
- route_mlp: int32 [4, 1024, 2], P('dp', ('expert', 'shard')), may hold values from 0 to 3, all different within a row
- prefix: int32 [4], P('dp'), may hold values from 102 to 512
- cotangent: bfloat16 [4, 1024, 2048], P('dp', ('expert', 'shard')), may hold values from -6 to 6
Outputs:
- output: bfloat16 [4, 1024, 2048], P('dp', ('expert', 'shard'))
- input_grad: float32 [4, 1024, 2048], P('dp', ('expert', 'shard'))
- gain_grad: float32 [2, 2048], replicated
- router_grad: float32 [2, 2048, 4], replicated
- kv_weight_grad: float32 [2048, 4096], P(('dp', 'expert', 'shard'))
- query_weight_grad: float32 [4, 2048, 2048], P('expert', ('dp', 'shard'))
- output_weight_grad: float32 [4, 2048, 2048], P('expert', ('dp', 'shard'))
- inner_weight_grad: float32 [4, 2048, 11264], P('expert', ('dp', 'shard'))
- outer_weight_grad: float32 [4, 5632, 2048], P('expert', ('dp', 'shard'))
The draws below stay inside these ranges and needn't reach their ends.
Inputs may be any that keep to these rules, and one draw needn't show every extreme that they name: `route_attn`: each token names 2 different experts in each route array. `route_mlp`: each token names 2 different experts in each route array. Keys before a sequence's prefix length are seen by every query of that sequence.
All inputs are finite; a program needn't handle non-finite values.
Results may differ from the reference program's by a relative error of at most 0.02.
Values may be sent and summed in bfloat16 or wider, within the bound.
A program may use at most 384 MiB of HBM per device.

```python
import jax
import jax.numpy as jnp
from jax import lax

D = 2048
HEADS = 16
HEAD_DIM = 128
FF = 5632
TOP = 2
TOK_DEV = 128
EXPERTS = 4
SEQS = 4
SEQ_LEN = 1024
CAP = 80
QW = 2048
KVW = 4096


def set_ends(array, own_key, low, top_value):
    longest = array.shape.index(max(array.shape))
    spots = []
    for shift in (0, 1):
        where = [jax.random.randint(jax.random.fold_in(own_key, axis), (), 0, length) for axis, length in enumerate(array.shape)]
        where[longest] = (where[longest] + shift) % array.shape[longest]
        spots.append(tuple(where))
    return array.at[spots[0]].set(low).at[spots[1]].set(top_value)


def shard_levels(rng, extent, split, smallest, largest):
    factor_of, own = 1.0, jax.random.fold_in(rng, 6)
    for dim, blocks in split:
        steps = jnp.exp(jax.random.uniform(jax.random.fold_in(own, dim), (blocks,), jnp.float32, smallest / len(split), largest / len(split)))
        factor_of = factor_of * jnp.repeat(steps, extent[dim] // blocks).reshape([-1 if axis == dim else 1 for axis in range(len(extent))])
    return factor_of


def distinct(rng, rows, number_of, top, lift):
    sequence = jax.random.permutation(jax.random.fold_in(rng, 1), number_of)
    boost = sequence
    for power in range(3):
        boost = boost * boost // number_of
    boost = boost * lift // number_of
    chance = jax.random.randint(jax.random.fold_in(rng, 2), (rows, number_of), 0, 4096) + boost
    fixed_rows = jax.random.permutation(jax.random.fold_in(rng, 3), rows)[jnp.arange(number_of) % rows]
    chance = jnp.where(jnp.arange(rows)[:, None] == fixed_rows[None, :], 1 << 14, chance)
    priority = chance * number_of + jnp.arange(number_of)
    return lax.top_k(priority.astype(jnp.int32), top)[1].astype(jnp.int32)


def bell_draw(stream_key, extent, spread, most, cuts=(), kind=jnp.bfloat16):
    entries = jax.random.normal(stream_key, extent, jnp.float32) * spread
    if len(cuts) > 0:
        entries = shard_levels(stream_key, extent, cuts, -0.22, 0.18) * entries
    return jnp.clip(entries, min=-most, max=most).astype(kind)


def setup_inputs(seed: int = 0) -> dict:
    splits = jax.random.split(jax.random.key(seed), 13)
    return {
        "tokens": bell_draw(splits[0], (SEQS, SEQ_LEN, D), 1.0, 6.0, ((0, 4), (1, 8))),
        "norm_gains": jnp.clip(1.0 + 0.1 * jax.random.normal(splits[1], (2, D), jnp.float32), 0.5, 1.5),
        "routers": bell_draw(splits[2], (2, D, EXPERTS), (2 * D) ** -0.5, 0.09375, (), jnp.float32),
        "kv_weight": bell_draw(splits[3], (D, KVW), D ** -0.5, 0.125, ((0, 32),)),
        "query_weight": bell_draw(splits[4], (EXPERTS, D, QW), D ** -0.5, 0.125, ((0, 4), (1, 8))),
        "output_weight": bell_draw(splits[5], (EXPERTS, QW, D), (max(D * 16 // SEQ_LEN, 1)) ** -0.5, 1.0, ((0, 4), (1, 8))),
        "inner_weight": bell_draw(splits[6], (EXPERTS, D, 2 * FF), D ** -0.5, 0.125, ((0, 4), (1, 8))),
        "outer_weight": bell_draw(splits[7], (EXPERTS, FF, D), FF ** -0.5, 0.078125, ((0, 4), (1, 8))),
        "route_attn": distinct(splits[8], SEQS * SEQ_LEN, EXPERTS, TOP, 4096).reshape((SEQS, SEQ_LEN, TOP)),
        "route_mlp": distinct(splits[9], SEQS * SEQ_LEN, EXPERTS, TOP, 4096).reshape((SEQS, SEQ_LEN, TOP)),
        "prefix": set_ends(jax.random.randint(splits[10], (SEQS,), SEQ_LEN // 10, SEQ_LEN // 2 + 1), jax.random.fold_in(splits[10], 1), SEQ_LEN // 10, (SEQ_LEN // 2 + 1) - 1).astype(jnp.int32),
        "cotangent": bell_draw(splits[11], (SEQS, SEQ_LEN, D), 1.0, 6.0, ((0, 4), (1, 8))),
    }


@jax.custom_vjp
def low(v):
    return lax.optimization_barrier(v.astype(jnp.bfloat16)).astype(jnp.float32)

@jax.custom_vjp
def low_back(v):
    return v

def low_keep(v):
    return (low(v), None)

def low_pass(kept, grad):
    return (grad,)

def back_keep(v):
    return (v, None)

def back_low(kept, grad):
    return (low(grad),)
low.defvjp(low_keep, low_pass)
low_back.defvjp(back_keep, back_low)
eps = 1e-05
finest = lax.Precision.HIGHEST

def matmul(first, second):
    return jnp.dot(first, second, precision=finest, preferred_element_type=jnp.float32)

def per_expert(slots, weight):
    return jnp.einsum('erd,edf->erf', slots, weight, precision=finest, preferred_element_type=jnp.float32)

def rms_scale(values, gain):
    factor = lax.rsqrt(lax.optimization_barrier(jnp.mean(values * values, axis=1, keepdims=True)) + eps)
    return values * factor * gain

def slot_plan(routes):
    blocks = routes.reshape(-1, TOK_DEV * TOP)
    count = blocks.shape[0]
    onehot = (blocks[:, :, None] == jnp.arange(EXPERTS, dtype=jnp.int32)[None, None, :]).astype(jnp.int32)
    before = jnp.cumsum(onehot, axis=1) - onehot
    rank = lax.optimization_barrier(jnp.sum(before * onehot, axis=2))
    kept = rank < CAP
    owner = jnp.arange(count, dtype=jnp.int32)[:, None]
    target = (blocks * count + owner) * CAP + rank
    target = jnp.where(kept, target, EXPERTS * count * CAP).astype(jnp.int32)
    return (target.reshape(-1), kept.reshape(-1, TOP).astype(jnp.float32), count)

def dispatch(rows, target, count):
    width = rows.shape[1]
    filled = jnp.zeros((EXPERTS * count * CAP, width), jnp.float32).at[target].add(rows, mode='drop')
    return filled.reshape(EXPERTS, count * CAP, width)

def collect(slots, target):
    width = slots.shape[2]
    return jnp.take(slots.reshape(-1, width), target, axis=0, mode='fill', fill_value=0.0)

def gates_of(normed, router, routes):
    logits = matmul(normed, router)
    picked = jnp.take_along_axis(logits, routes, axis=1)
    return jax.nn.softmax(picked, axis=1)

def attend_head(query, key, value, limit):
    scale = HEAD_DIM ** (-0.5)
    scores = low_back(matmul(query, key.T) * scale)
    spot = jnp.arange(query.shape[0], dtype=jnp.int32) // TOP
    column = jnp.arange(key.shape[0], dtype=jnp.int32)
    seen = (column[None, :] <= spot[:, None]) | (column[None, :] < limit)
    weights = jax.nn.softmax(jnp.where(seen, scores, -jnp.inf), axis=1)
    return matmul(low(weights), value)

def attend_sequence(items):
    query, key, value, limit = items

    def one_head(parts):
        return attend_head(parts[0], parts[1], parts[2], limit)
    result = lax.map(jax.checkpoint(one_head), (query.transpose(1, 0, 2), key.transpose(1, 0, 2), value.transpose(1, 0, 2)))
    return result.transpose(1, 0, 2)

def reference(tokens, norm_gains, routers, kv_weight, query_weight, output_weight, inner_weight, outer_weight, route_attn, route_mlp, prefix, cotangent):
    pairs_attn = route_attn.reshape(-1, TOP)
    pairs_mlp = route_mlp.reshape(-1, TOP)
    target_attn, keep_attn, count = slot_plan(pairs_attn)
    target_mlp, keep_mlp, count = slot_plan(pairs_mlp)

    def forward(inputs, gains, router_pair, kv_full, query_full, output_full, inner_full, outer_full):
        normed_attn = low(rms_scale(inputs, gains[0]))
        kv = low_back(low(matmul(normed_attn, kv_full)))
        gate_attn = gates_of(normed_attn, router_pair[0], pairs_attn)
        rows_attn = low_back(jnp.repeat(normed_attn, TOP, axis=0))
        slots_attn = dispatch(rows_attn, target_attn, count)
        query_slots = low_back(low(per_expert(slots_attn, query_full)))
        queries = collect(query_slots, target_attn)
        heads_query = queries.reshape(SEQS, SEQ_LEN * TOP, HEADS, HEAD_DIM)
        keys = kv[:, :QW].reshape(SEQS, SEQ_LEN, HEADS, HEAD_DIM)
        values = kv[:, QW:].reshape(SEQS, SEQ_LEN, HEADS, HEAD_DIM)
        attended = lax.map(attend_sequence, (heads_query, keys, values, prefix))
        attended = low_back(low(attended.reshape(-1, QW)))
        output_slots = dispatch(attended, target_attn, count)
        attn_slots = low_back(low(per_expert(output_slots, output_full)))
        attn_pairs = collect(attn_slots, target_attn).reshape(-1, TOP, D)
        hidden_state = inputs + lax.optimization_barrier(jnp.sum((keep_attn * gate_attn)[:, :, None] * attn_pairs, axis=1))
        normed_mlp = low(rms_scale(hidden_state, gains[1]))
        gate_mlp = gates_of(normed_mlp, router_pair[1], pairs_mlp)
        rows_mlp = low_back(jnp.repeat(normed_mlp, TOP, axis=0))
        slots_mlp = dispatch(rows_mlp, target_mlp, count)
        gate_up = low_back(per_expert(slots_mlp, inner_full))
        inner = low(jax.nn.silu(gate_up[:, :, :FF]) * gate_up[:, :, FF:])
        mlp_slots = low_back(low(per_expert(inner, outer_full)))
        mlp_pairs = collect(mlp_slots, target_mlp).reshape(-1, TOP, D)
        return hidden_state + lax.optimization_barrier(jnp.sum((keep_mlp * gate_mlp)[:, :, None] * mlp_pairs, axis=1))
    primals = (tokens.reshape(-1, D).astype(jnp.float32), norm_gains, routers, kv_weight.astype(jnp.float32), query_weight.astype(jnp.float32), output_weight.astype(jnp.float32), inner_weight.astype(jnp.float32), outer_weight.astype(jnp.float32))
    result, pullback = jax.vjp(forward, *primals)
    grads = pullback(cotangent.reshape(-1, D).astype(jnp.float32))
    output = result.astype(jnp.bfloat16).reshape(SEQS, SEQ_LEN, D)
    input_grad = grads[0].reshape(SEQS, SEQ_LEN, D)
    return (output, input_grad, grads[1], grads[2], grads[3], grads[4], grads[5], grads[6], grads[7])
```

```python
import functools

import jax
import jax.numpy as jnp
from jax import lax
from jax.experimental import pallas as pl
from jax.experimental.pallas import tpu as pltpu
from jax.sharding import PartitionSpec as P

D = 2048
HEADS = 16
HEAD_DIM = 128
FF = 5632
F32 = jnp.float32
BF16 = jnp.bfloat16

eps = 1e-05
finest = lax.Precision.HIGHEST


def matmul(first, second):
    return jnp.dot(first, second, preferred_element_type=F32)


def precise(first, second):
    return jnp.dot(first, second, precision=finest, preferred_element_type=F32)


def router_back(gates, grad_gates, chosen, normed, router):
    grad_pick = gates * (grad_gates - jnp.sum(grad_gates * gates, axis=1, keepdims=True))
    grad_logit = jnp.sum(chosen * grad_pick[:, :, None], axis=1)
    router_grad = precise(normed.astype(F32).T, grad_logit)
    return (router_grad, precise(grad_logit, router.T))


def norm_back(values, factor, gain, grad_normed):
    unit = values * factor
    gain_grad = jnp.sum(grad_normed * unit, axis=0)
    grad_unit = grad_normed * gain
    grad_values = factor * (grad_unit - unit * jnp.mean(grad_unit * unit, axis=1, keepdims=True))
    return (grad_values, gain_grad)


def gates_of(normed, router, chosen):
    logits = precise(normed.astype(F32), router)
    picked = jnp.sum(chosen * logits[:, None, :], axis=2)
    return jax.nn.softmax(picked, axis=1)


def slot_plan(routes, experts, capacity):
    pairs = routes.reshape(-1)
    onehot = (pairs[:, None] == jnp.arange(experts, dtype=jnp.int32)[None, :]).astype(jnp.int32)
    before = jnp.cumsum(onehot, axis=0) - onehot
    rank = jnp.sum(before * onehot, axis=1)
    kept = rank < capacity
    target = pairs * capacity + rank
    place = (target[None, :] == jnp.arange(experts * capacity, dtype=jnp.int32)[:, None]) & kept[
        None, :
    ]
    place = place.astype(jnp.float32)
    merged = place.reshape(experts * capacity, -1, 2).sum(axis=2)
    keep = kept.astype(jnp.float32).reshape(-1, 2)
    chosen = onehot.astype(jnp.float32).reshape(-1, 2, experts)
    return (place.astype(jnp.bfloat16), merged.astype(jnp.bfloat16), keep, chosen)


def from_slots(place, slots):
    flat = slots.reshape(place.shape[0], -1)
    return jnp.einsum("sp,sw->pw", place, flat, preferred_element_type=jnp.float32)


def send_out(buffer):
    return lax.all_to_all(buffer, "expert", split_axis=0, concat_axis=0, tiled=True)


def send_back(buffer):
    return lax.all_to_all(buffer, "expert", split_axis=0, concat_axis=0, tiled=True)


def exclusive_count(flags):
    size = flags.shape[-1]
    earlier = jnp.arange(size)[:, None] < jnp.arange(size)[None, :]
    return jnp.dot(flags.astype(BF16), earlier.astype(BF16), preferred_element_type=F32)


Q_ROWS = 256


def head_mask(tile, rows, tokens, keys, prefix):
    first = lax.rem(tile * rows, tokens)
    spot = first + lax.broadcasted_iota(jnp.int32, (rows, keys), 0)
    column = lax.broadcasted_iota(jnp.int32, (rows, keys), 1)
    return (column <= spot) | (column < prefix)


def attend_kernel(tokens, prefix_ref, q_ref, k_ref, v_ref, out_ref, lse_ref):
    tile = pl.program_id(1)
    rows, keys = q_ref.shape[0], k_ref.shape[0]
    scores = lax.dot_general(q_ref[...], k_ref[...], (((1,), (1,)), ((), ())), preferred_element_type=F32)
    scores = scores * (HEAD_DIM ** (-0.5))
    scores = jnp.where(head_mask(tile, rows, tokens, keys, prefix_ref[0]), scores, -jnp.inf)
    highest = jnp.max(scores, axis=1, keepdims=True)
    expo = jnp.exp(scores - highest)
    total = jnp.sum(expo, axis=1, keepdims=True)
    weights = (expo / total).astype(BF16)
    out_ref[...] = jnp.dot(weights, v_ref[...], preferred_element_type=F32).astype(BF16)
    lse_ref[0] = highest + jnp.log(total)


def attend(prefix, queries, keys, values):
    pairs, width = queries.shape
    seq = keys.shape[0]
    heads = width // HEAD_DIM
    tiles = pairs // Q_ROWS
    return pl.pallas_call(
        functools.partial(attend_kernel, pairs // 2),
        out_shape=(
            jax.ShapeDtypeStruct((pairs, width), BF16),
            jax.ShapeDtypeStruct((heads, pairs, 1), F32),
        ),
        grid_spec=pltpu.PrefetchScalarGridSpec(
            num_scalar_prefetch=1,
            grid=(heads, tiles),
            in_specs=[
                pl.BlockSpec((Q_ROWS, HEAD_DIM), lambda h, i, p: (i, h)),
                pl.BlockSpec((seq, HEAD_DIM), lambda h, i, p: (0, h)),
                pl.BlockSpec((seq, HEAD_DIM), lambda h, i, p: (0, h)),
            ],
            out_specs=[
                pl.BlockSpec((Q_ROWS, HEAD_DIM), lambda h, i, p: (i, h)),
                pl.BlockSpec((1, Q_ROWS, 1), lambda h, i, p: (h, i, 0)),
            ],
        ),
        compiler_params=pltpu.CompilerParams(vmem_limit_bytes=32 * 1024 * 1024),
        cost_estimate=pl.CostEstimate(
            flops=4 * pairs * seq * width, transcendentals=pairs * seq * heads, bytes_accessed=8 * pairs * width
        ),
        name="attend",
    )(prefix, queries, keys, values)


def attend_back_kernel(
    tokens, prefix_ref, q_ref, up_ref, k_ref, v_ref, lse_ref, dq_ref, dk_ref, dv_ref, dk_acc, dv_acc
):
    tile = pl.program_id(1)
    rows, keys = q_ref.shape[0], k_ref.shape[0]
    scale = HEAD_DIM ** (-0.5)

    @pl.when(tile == 0)
    def _():
        dk_acc[...] = jnp.zeros_like(dk_acc)
        dv_acc[...] = jnp.zeros_like(dv_acc)

    scores = lax.dot_general(q_ref[...], k_ref[...], (((1,), (1,)), ((), ())), preferred_element_type=F32)
    scores = jnp.where(head_mask(tile, rows, tokens, keys, prefix_ref[0]), scores * scale, -jnp.inf)
    probs = jnp.exp(scores - lse_ref[0])
    upstream = up_ref[...]
    grad_probs = lax.dot_general(upstream, v_ref[...], (((1,), (1,)), ((), ())), preferred_element_type=F32)
    delta = jnp.sum(grad_probs * probs, axis=1, keepdims=True)
    grad_scores = (probs * (grad_probs - delta)).astype(BF16)
    dq_ref[...] = (jnp.dot(grad_scores, k_ref[...], preferred_element_type=F32) * scale).astype(BF16)
    dk_acc[...] += lax.dot_general(grad_scores, q_ref[...], (((0,), (0,)), ((), ())), preferred_element_type=F32)
    dv_acc[...] += lax.dot_general(
        probs.astype(BF16), upstream, (((0,), (0,)), ((), ())), preferred_element_type=F32
    )

    @pl.when(tile == pl.num_programs(1) - 1)
    def _():
        dk_ref[...] = (dk_acc[...] * scale).astype(BF16)
        dv_ref[...] = dv_acc[...].astype(BF16)


def attend_back(prefix, queries, upstream, keys, values, lse):
    pairs, width = queries.shape
    seq = keys.shape[0]
    heads = width // HEAD_DIM
    tiles = pairs // Q_ROWS
    by_tile = pl.BlockSpec((Q_ROWS, HEAD_DIM), lambda h, i, p: (i, h))
    by_head = pl.BlockSpec((seq, HEAD_DIM), lambda h, i, p: (0, h))
    return pl.pallas_call(
        functools.partial(attend_back_kernel, pairs // 2),
        out_shape=(
            jax.ShapeDtypeStruct((pairs, width), BF16),
            jax.ShapeDtypeStruct((seq, width), BF16),
            jax.ShapeDtypeStruct((seq, width), BF16),
        ),
        grid_spec=pltpu.PrefetchScalarGridSpec(
            num_scalar_prefetch=1,
            grid=(heads, tiles),
            in_specs=[
                by_tile,
                by_tile,
                by_head,
                by_head,
                pl.BlockSpec((1, Q_ROWS, 1), lambda h, i, p: (h, i, 0)),
            ],
            out_specs=[by_tile, by_head, by_head],
            scratch_shapes=[pltpu.VMEM((seq, HEAD_DIM), F32), pltpu.VMEM((seq, HEAD_DIM), F32)],
        ),
        compiler_params=pltpu.CompilerParams(vmem_limit_bytes=32 * 1024 * 1024),
        cost_estimate=pl.CostEstimate(
            flops=10 * pairs * seq * width, transcendentals=pairs * seq * heads, bytes_accessed=8 * pairs * width
        ),
        name="attend_back",
    )(prefix, queries, upstream, keys, values, lse)


PLANE = ("expert", "shard")
GROUP = ("dp", "shard")
ALL = ("dp", "expert", "shard")


def gather_rows(rows, axes):
    return lax.all_gather(rows, axes, axis=0, tiled=True)


def sum_rows(partial, axes):
    pieces = lax.all_to_all(partial, axes, split_axis=0, concat_axis=0, tiled=True)
    count = lax.axis_size(axes)
    return jnp.sum(pieces.reshape(count, -1, partial.shape[1]).astype(F32), axis=0)


def exchange(blocks, axes):
    return lax.all_to_all(blocks, axes, split_axis=0, concat_axis=0, tiled=True)


def per_device(
    tokens,
    norm_gains,
    routers,
    kv_weight,
    query_weight,
    output_weight,
    inner_weight,
    outer_weight,
    route_attn,
    route_mlp,
    prefix,
    cotangent,
):
    tok = tokens.shape[1]
    experts = lax.axis_size("expert")
    depth = lax.axis_size("dp")
    sides = lax.axis_size("shard")
    plane = experts * sides
    group = depth * sides
    everyone = plane * depth
    capacity = 5 * tok // (2 * experts)
    seq = plane * tok
    qwidth = HEADS * HEAD_DIM
    own = qwidth // plane
    half = FF // group
    my_expert = lax.axis_index("expert")

    inputs = tokens[0].astype(F32)
    factor_attn = lax.rsqrt(jnp.mean(inputs * inputs, axis=1, keepdims=True) + eps)
    normed_attn = (inputs * factor_attn * norm_gains[0]).astype(BF16)
    grad_rows = cotangent[0]

    expert_ids = jnp.arange(experts, dtype=jnp.int32)
    chosen_attn = (route_attn[0][:, :, None] == expert_ids).astype(F32)
    chosen_mlp = (route_mlp[0][:, :, None] == expert_ids).astype(F32)

    def keep_of(chosen):
        flags = jnp.sum(chosen, axis=1)
        rank = exclusive_count(flags.T).T
        return jnp.sum(chosen * (rank < capacity).astype(F32)[:, None, :], axis=2)

    keep_attn = keep_of(chosen_attn)
    keep_mlp = keep_of(chosen_mlp)
    gate_attn = gates_of(normed_attn, routers[0], chosen_attn)
    weight_attn = keep_attn * gate_attn

    kv_parts = kv_weight.reshape(-1, 2, plane, own).transpose(2, 0, 1, 3)
    kv_mine = exchange(kv_parts, PLANE).reshape(-1, 2 * own)
    kv_mine = gather_rows(kv_mine, "dp")
    query_parts = query_weight[0].reshape(-1, plane, own).transpose(1, 0, 2)
    query_mine = exchange(query_parts, PLANE)
    rows_each = query_parts.shape[1]
    query_mine = lax.all_gather(query_mine.reshape(experts, sides * rows_each, own), "dp", axis=1, tiled=True)
    output_all = lax.all_gather(output_weight[0], "dp", axis=0, tiled=False)
    output_mine = exchange(output_all, "expert")

    normed_seq = gather_rows(normed_attn, PLANE)
    meta = jnp.concatenate(
        [weight_attn[:, :, None] * chosen_attn, keep_attn[:, :, None] * chosen_attn], axis=1
    ).reshape(tok, -1)
    meta_seq = gather_rows(meta, PLANE).reshape(seq, 2, 2, experts)
    weigh = meta_seq[:, 0]
    pick = meta_seq[:, 1]

    kv_seq = matmul(normed_seq, kv_mine).astype(BF16)
    keys, values = kv_seq[:, :own], kv_seq[:, own:]
    every_query = jnp.einsum("td,edq->teq", normed_seq, query_mine, preferred_element_type=F32)
    queries = [
        sum(pick[:, choice, e, None] * every_query[:, e] for e in range(experts)).astype(BF16) for choice in (0, 1)
    ]
    queries = jnp.concatenate(queries, axis=0)
    attended, lse = attend(prefix, queries, keys, values)
    pair_attended = attended.reshape(2, seq, own).astype(F32)
    mixed = jnp.stack(
        [
            (weigh[:, 0, e, None] * pair_attended[0] + weigh[:, 1, e, None] * pair_attended[1]).astype(BF16)
            for e in range(experts)
        ],
        axis=1,
    )
    attn_part = jnp.einsum("teq,eqd->td", mixed, output_mine, preferred_element_type=F32).astype(BF16)
    hidden_state = inputs + sum_rows(attn_part, PLANE)
    factor_mlp = lax.rsqrt(jnp.mean(hidden_state * hidden_state, axis=1, keepdims=True) + eps)
    normed_mlp = (hidden_state * factor_mlp * norm_gains[1]).astype(BF16)
    gate_mlp = gates_of(normed_mlp, routers[1], chosen_mlp)

    inner_parts = inner_weight[0].reshape(-1, 2, group, half).transpose(2, 0, 1, 3)
    inner_mine = exchange(inner_parts, GROUP).reshape(-1, 2 * half)
    outer_mine = outer_weight[0]
    gated = jnp.concatenate(
        [jnp.sum(chosen_mlp, axis=1), jnp.sum(gate_mlp[:, :, None] * chosen_mlp, axis=1)], axis=1
    )
    gated_all = gather_rows(gated, ALL)
    flags = lax.dynamic_index_in_dim(gated_all, my_expert, 1, keepdims=False).reshape(everyone, tok)
    gate_all = lax.dynamic_index_in_dim(gated_all, my_expert + experts, 1, keepdims=False).reshape(everyone, tok)
    normed_all = gather_rows(normed_mlp, ALL).reshape(everyone, tok, D)
    grad_all = gather_rows(grad_rows, ALL).reshape(everyone, tok, D)
    rank = exclusive_count(flags)
    slot_ids = jnp.arange(capacity, dtype=F32)
    place = (rank[:, None, :] == slot_ids[None, :, None]) & (flags[:, None, :] > 0)
    slot_gate = jnp.sum(jnp.where(place, gate_all[:, None, :], 0.0), axis=2).reshape(-1, 1)
    place = place.astype(BF16)

    def to_slots(rows):
        return jnp.einsum("bst,btd->bsd", place, rows, preferred_element_type=F32).astype(BF16).reshape(-1, D)

    def to_tokens(slots):
        slots = slots.reshape(everyone, capacity, -1)
        return jnp.einsum("bst,bsd->btd", place, slots, preferred_element_type=F32)

    slots_mlp = to_slots(normed_all)
    slots_grad = to_slots(grad_all)
    gate_up = matmul(slots_mlp, inner_mine)
    gate_part = gate_up[:, :half]
    up_part = gate_up[:, half:]
    sigmoid_gate = jax.nn.sigmoid(gate_part)
    activated = gate_part * sigmoid_gate
    inner = (activated * up_part).astype(BF16)
    out_part = (matmul(inner, outer_mine) * slot_gate).astype(BF16)
    out_part = to_tokens(out_part).astype(BF16).reshape(-1, D)
    raw_inner = jnp.einsum("rd,fd->rf", slots_grad, outer_mine, preferred_element_type=F32)
    gate_dot = jnp.sum(raw_inner * inner.astype(F32), axis=1, keepdims=True)
    grad_inner = raw_inner * slot_gate
    grad_gate = grad_inner * up_part * (sigmoid_gate * (1.0 + gate_part * (1.0 - sigmoid_gate)))
    grad_up = grad_inner * activated
    grad_gate_up = jnp.concatenate([grad_gate, grad_up], axis=1).astype(BF16)
    scaled_inner = (inner.astype(F32) * slot_gate).astype(BF16)
    outer_grad = jnp.einsum("rf,rd->fd", scaled_inner, slots_grad, preferred_element_type=F32)
    inner_grad = jnp.einsum("rd,rf->df", slots_mlp, grad_gate_up, preferred_element_type=F32).astype(BF16)
    grad_part = jnp.einsum("rf,df->rd", grad_gate_up, inner_mine, preferred_element_type=F32).astype(BF16)
    grad_part = to_tokens(grad_part).astype(BF16).reshape(-1, D)

    grad_normed_mlp = sum_rows(grad_part, ALL)
    dot_tokens = jnp.sum(place.astype(F32) * gate_dot.reshape(everyone, capacity, 1), axis=1)
    dot_mine = lax.all_to_all(dot_tokens, ALL, split_axis=0, concat_axis=0, tiled=True)
    dot_mine = jnp.sum(dot_mine.reshape(depth, experts, sides, tok), axis=(0, 2))
    grad_gate_mlp = keep_mlp * jnp.sum(chosen_mlp * dot_mine.T[:, None, :], axis=2)
    result = hidden_state + sum_rows(out_part, ALL)
    output = result.astype(BF16)[None]
    inner_grad = inner_grad.reshape(group, -1, 2 * half)
    inner_grad = exchange(inner_grad, GROUP)
    inner_grad = inner_grad.reshape(group, -1, 2, half).transpose(1, 2, 0, 3).reshape(-1, 2 * FF).astype(F32)

    router_grad_mlp, router_part_mlp = router_back(
        gate_mlp, grad_gate_mlp, chosen_mlp, normed_mlp, routers[1]
    )
    grad_normed_mlp = grad_normed_mlp + router_part_mlp
    grad_hidden, gain_grad_mlp = norm_back(hidden_state, factor_mlp, norm_gains[1], grad_normed_mlp)
    grad_hidden = grad_hidden + grad_rows.astype(F32)

    hidden_seq = gather_rows(grad_hidden.astype(BF16), PLANE)
    raw_attended = jnp.einsum("td,eqd->teq", hidden_seq, output_mine, preferred_element_type=F32)
    raw_pair = [sum(pick[:, choice, e, None] * raw_attended[:, e] for e in range(experts)) for choice in (0, 1)]
    gate_dots = jnp.stack([jnp.sum(raw_pair[c] * pair_attended[c], axis=1) for c in (0, 1)], axis=1)
    weight_seq = jnp.sum(weigh, axis=2)
    upstream = jnp.concatenate([(weight_seq[:, c, None] * raw_pair[c]).astype(BF16) for c in (0, 1)], axis=0)
    grad_queries, grad_keys, grad_values = attend_back(prefix, queries, upstream, keys, values, lse)
    pair_grads = grad_queries.reshape(2, seq, own)
    spread = jnp.stack(
        [
            (pick[:, 0, e, None] * pair_grads[0] + pick[:, 1, e, None] * pair_grads[1]).astype(BF16)
            for e in range(experts)
        ],
        axis=1,
    )
    row_part = jnp.einsum("teq,edq->td", spread, query_mine, preferred_element_type=F32)
    grad_kv = jnp.concatenate([grad_keys, grad_values], axis=1)
    row_part = row_part + jnp.einsum("tk,dk->td", grad_kv, kv_mine, preferred_element_type=F32)
    grad_normed_attn = sum_rows(row_part.astype(BF16), PLANE)
    dots_mine = sum_rows(gate_dots, PLANE)
    grad_gate_attn = keep_attn * dots_mine

    output_grad = jnp.einsum("teq,td->eqd", mixed, hidden_seq, preferred_element_type=F32).astype(BF16)
    output_grad = exchange(output_grad, "expert")
    output_grad = sum_rows(output_grad.reshape(depth * own, D), "dp")
    query_grad = jnp.einsum("td,teq->deq", normed_seq, spread, preferred_element_type=F32).astype(BF16)
    kv_grad = jnp.einsum("td,tk->dk", normed_seq, grad_kv, preferred_element_type=F32).astype(BF16)
    query_grad = sum_rows(query_grad.reshape(D, -1), "dp").astype(BF16)
    kv_grad = sum_rows(kv_grad, "dp").astype(BF16)
    query_grad = query_grad.reshape(sides, rows_each, experts, own).transpose(2, 0, 1, 3).reshape(plane, rows_each, own)
    query_grad = exchange(query_grad, PLANE).transpose(1, 0, 2).reshape(rows_each, qwidth).astype(F32)
    kv_grad = exchange(kv_grad.reshape(plane, -1, 2 * own), PLANE)
    kv_grad = kv_grad.reshape(plane, -1, 2, own).transpose(1, 2, 0, 3).reshape(-1, 2 * qwidth).astype(F32)

    router_grad_attn, router_part_attn = router_back(
        gate_attn, grad_gate_attn, chosen_attn, normed_attn, routers[0]
    )
    grad_normed_attn = grad_normed_attn + router_part_attn
    grad_inputs, gain_grad_attn = norm_back(inputs, factor_attn, norm_gains[0], grad_normed_attn)
    grad_inputs = grad_inputs + grad_hidden
    gain_grad, router_grad = lax.psum(
        (
            jnp.stack([gain_grad_attn, gain_grad_mlp]),
            jnp.stack([router_grad_attn, router_grad_mlp]),
        ),
        ("dp", "expert", "shard"),
    )
    return (
        output,
        grad_inputs[None],
        gain_grad,
        router_grad,
        kv_grad,
        query_grad[None],
        output_grad[None],
        inner_grad[None],
        outer_grad[None],
    )


def per_device_gathered(
    tokens,
    norm_gains,
    routers,
    kv_weight,
    query_weight,
    output_weight,
    inner_weight,
    outer_weight,
    route_attn,
    route_mlp,
    prefix,
    cotangent,
):
    tok_count = tokens.shape[1]
    experts = lax.axis_size("expert")
    capacity = 5 * tok_count // (2 * experts)
    qwidth = HEADS * HEAD_DIM
    scale = HEAD_DIM ** (-0.5)
    inputs = tokens[0].astype(jnp.float32)
    factor_attn = lax.rsqrt(jnp.mean(inputs * inputs, axis=1, keepdims=True) + eps)
    normed_attn = (inputs * factor_attn * norm_gains[0]).astype(jnp.bfloat16)
    kv_full = lax.all_gather(kv_weight, ("dp", "expert", "shard"), axis=0, tiled=True)
    keys_local = matmul(normed_attn, kv_full).astype(jnp.bfloat16)
    keys_all = lax.all_gather(keys_local, ("expert", "shard"), axis=0, tiled=True)
    gathered = (
        lax.all_gather(query_weight, ("dp", "shard"), axis=1, tiled=True),
        lax.all_gather(output_weight, ("dp", "shard"), axis=1, tiled=True),
        lax.all_gather(inner_weight, ("dp", "shard"), axis=1, tiled=True),
        lax.all_gather(outer_weight, ("dp", "shard"), axis=1, tiled=True),
    )
    query_full, output_full, inner_full, outer_full = (
        gathered[0][0],
        gathered[1][0],
        gathered[2][0],
        gathered[3][0],
    )
    place_attn, merged_attn, keep_attn, chosen_attn = slot_plan(route_attn[0], experts, capacity)
    gate_attn = gates_of(normed_attn, routers[0], chosen_attn)
    slots_attn = send_out(
        matmul(merged_attn, normed_attn).astype(jnp.bfloat16).reshape(experts, capacity, D)
    ).reshape(-1, D)
    query_back = send_back(
        matmul(slots_attn, query_full).astype(jnp.bfloat16).reshape(experts, capacity, qwidth)
    )
    queries = from_slots(place_attn, query_back).astype(jnp.bfloat16)
    offset = lax.axis_index(("expert", "shard")) * tok_count
    spot = offset + jnp.arange(2 * tok_count, dtype=jnp.int32) // 2
    column = jnp.arange(keys_all.shape[0], dtype=jnp.int32)
    visible = (column[None, :] <= spot[:, None]) | (column[None, :] < prefix[0])

    def head_parts(head):
        query = lax.dynamic_slice_in_dim(queries, head * HEAD_DIM, HEAD_DIM, 1)
        key = lax.dynamic_slice_in_dim(keys_all, head * HEAD_DIM, HEAD_DIM, 1)
        value = lax.dynamic_slice_in_dim(keys_all, qwidth + head * HEAD_DIM, HEAD_DIM, 1)
        return (query, key, value)

    def head_scores(query, key):
        scores = jnp.einsum("pd,kd->pk", query, key, preferred_element_type=jnp.float32) * scale
        return jnp.where(visible, scores, -jnp.inf)

    def head_forward(head):
        query, key, value = head_parts(head)
        scores = head_scores(query, key)
        highest = jnp.max(scores, axis=1, keepdims=True)
        expo = jnp.exp(scores - highest)
        total = jnp.sum(expo, axis=1, keepdims=True)
        weights = (expo / total).astype(jnp.bfloat16)
        result = jnp.dot(weights, value, preferred_element_type=jnp.float32).astype(jnp.bfloat16)
        return (result, (highest + jnp.log(total))[:, 0])

    head_outs, log_totals = lax.map(head_forward, jnp.arange(HEADS))
    attended = head_outs.transpose(1, 0, 2).reshape(-1, qwidth)
    output_slots = send_out(
        matmul(place_attn, attended).astype(jnp.bfloat16).reshape(experts, capacity, qwidth)
    ).reshape(-1, qwidth)
    attn_back = send_back(
        matmul(output_slots, output_full).astype(jnp.bfloat16).reshape(experts, capacity, D)
    )
    attn_pairs = from_slots(place_attn, attn_back).reshape(tok_count, 2, D)
    weight_attn = keep_attn * gate_attn
    hidden_state = inputs + jnp.sum(weight_attn[:, :, None] * attn_pairs, axis=1)
    factor_mlp = lax.rsqrt(jnp.mean(hidden_state * hidden_state, axis=1, keepdims=True) + eps)
    normed_mlp = (hidden_state * factor_mlp * norm_gains[1]).astype(jnp.bfloat16)
    place_mlp, merged_mlp, keep_mlp, chosen_mlp = slot_plan(route_mlp[0], experts, capacity)
    gate_mlp = gates_of(normed_mlp, routers[1], chosen_mlp)
    slots_mlp = send_out(
        matmul(merged_mlp, normed_mlp).astype(jnp.bfloat16).reshape(experts, capacity, D)
    ).reshape(-1, D)
    gate_up = matmul(slots_mlp, inner_full)
    gate_part = gate_up[:, :FF]
    up_part = gate_up[:, FF:]
    activated = jax.nn.silu(gate_part)
    inner = (activated * up_part).astype(jnp.bfloat16)
    mlp_back = send_back(
        matmul(inner, outer_full).astype(jnp.bfloat16).reshape(experts, capacity, D)
    )
    mlp_pairs = from_slots(place_mlp, mlp_back).reshape(tok_count, 2, D)
    weight_mlp = keep_mlp * gate_mlp
    result = hidden_state + jnp.sum(weight_mlp[:, :, None] * mlp_pairs, axis=1)
    output = result.astype(jnp.bfloat16)[None]
    regathered = (
        lax.all_gather(query_weight, ("dp", "shard"), axis=1, tiled=True),
        lax.all_gather(output_weight, ("dp", "shard"), axis=1, tiled=True),
        lax.all_gather(inner_weight, ("dp", "shard"), axis=1, tiled=True),
        lax.all_gather(outer_weight, ("dp", "shard"), axis=1, tiled=True),
    )
    query_full, output_full, inner_full, outer_full = (
        regathered[0][0],
        regathered[1][0],
        regathered[2][0],
        regathered[3][0],
    )
    grad = cotangent[0].astype(jnp.float32)
    grad_gate_mlp = keep_mlp * jnp.sum(grad[:, None, :] * mlp_pairs, axis=2)
    grad_mlp_pairs = (weight_mlp[:, :, None] * grad[:, None, :]).astype(jnp.bfloat16).reshape(-1, D)
    grad_mlp_slots = send_out(
        matmul(place_mlp, grad_mlp_pairs).astype(jnp.bfloat16).reshape(experts, capacity, D)
    ).reshape(-1, D)
    grad_inner = jnp.einsum(
        "rd,fd->rf", grad_mlp_slots, outer_full, preferred_element_type=jnp.float32
    )
    sigmoid_gate = jax.nn.sigmoid(gate_part)
    grad_gate = grad_inner * up_part * (sigmoid_gate * (1.0 + gate_part * (1.0 - sigmoid_gate)))
    grad_up = grad_inner * activated
    grad_gate_up = jnp.concatenate([grad_gate, grad_up], axis=1).astype(jnp.bfloat16)
    grad_row_mlp = send_back(
        jnp.einsum("rf,df->rd", grad_gate_up, inner_full, preferred_element_type=jnp.float32)
        .astype(jnp.bfloat16)
        .reshape(experts, capacity, D)
    )
    piece = inner
    outer_grad = lax.psum_scatter(
        jnp.einsum("rf,rd->fd", piece, grad_mlp_slots, preferred_element_type=jnp.float32).astype(
            jnp.bfloat16
        ),
        ("dp", "shard"),
        scatter_dimension=0,
        tiled=True,
    ).astype(jnp.float32)
    piece = slots_mlp
    inner_grad = lax.psum_scatter(
        jnp.einsum("rd,rf->df", piece, grad_gate_up, preferred_element_type=jnp.float32).astype(
            jnp.bfloat16
        ),
        ("dp", "shard"),
        scatter_dimension=0,
        tiled=True,
    ).astype(jnp.float32)
    grad_normed_mlp = from_slots(merged_mlp, grad_row_mlp)
    router_grad_mlp, router_part_mlp = router_back(
        gate_mlp, grad_gate_mlp, chosen_mlp, normed_mlp, routers[1]
    )
    grad_normed_mlp = grad_normed_mlp + router_part_mlp
    grad_hidden, gain_grad_mlp = norm_back(hidden_state, factor_mlp, norm_gains[1], grad_normed_mlp)
    grad_hidden = grad_hidden + grad
    grad_gate_attn = keep_attn * jnp.sum(grad_hidden[:, None, :] * attn_pairs, axis=2)
    grad_attn_pairs = (
        (weight_attn[:, :, None] * grad_hidden[:, None, :]).astype(jnp.bfloat16).reshape(-1, D)
    )
    grad_attn_slots = send_out(
        matmul(place_attn, grad_attn_pairs).astype(jnp.bfloat16).reshape(experts, capacity, D)
    ).reshape(-1, D)
    grad_out_back = send_back(
        jnp.einsum("rd,qd->rq", grad_attn_slots, output_full, preferred_element_type=jnp.float32)
        .astype(jnp.bfloat16)
        .reshape(experts, capacity, qwidth)
    )
    grad_attended = from_slots(place_attn, grad_out_back).astype(jnp.bfloat16)
    output_grad_term = jnp.einsum(
        "rq,rd->qd", output_slots, grad_attn_slots, preferred_element_type=jnp.float32
    )
    seq_len = keys_all.shape[0]

    def head_backward(carry, head):
        kv_terms, query_terms = carry
        query, key, value = head_parts(head)
        upstream = lax.dynamic_slice_in_dim(grad_attended, head * HEAD_DIM, HEAD_DIM, 1)
        log_total = lax.dynamic_index_in_dim(log_totals, head, 0, keepdims=False)
        probs = jnp.exp(head_scores(query, key) - log_total[:, None])
        grad_probs = jnp.einsum("pd,kd->pk", upstream, value, preferred_element_type=jnp.float32)
        delta = jnp.sum(grad_probs * probs, axis=1, keepdims=True)
        grad_scores = (probs * (grad_probs - delta)).astype(jnp.bfloat16)
        grad_query = jnp.dot(grad_scores, key, preferred_element_type=jnp.float32) * scale
        grad_key = (
            jnp.einsum("pk,pd->kd", grad_scores, query, preferred_element_type=jnp.float32) * scale
        )
        grad_value = jnp.einsum(
            "pk,pd->kd", probs.astype(jnp.bfloat16), upstream, preferred_element_type=jnp.float32
        )
        kv_terms = lax.dynamic_update_slice_in_dim(kv_terms, grad_key, head * HEAD_DIM, 1)
        kv_terms = lax.dynamic_update_slice_in_dim(
            kv_terms, grad_value, qwidth + head * HEAD_DIM, 1
        )
        query_terms = lax.dynamic_update_slice_in_dim(query_terms, grad_query, head * HEAD_DIM, 1)
        return ((kv_terms, query_terms), None)

    start_carry = (
        jnp.zeros((seq_len, 2 * qwidth), jnp.float32),
        jnp.zeros((2 * tok_count, qwidth), jnp.float32),
    )
    (grad_kv_terms, grad_query_terms), unused = lax.scan(
        head_backward, start_carry, jnp.arange(HEADS)
    )
    grad_queries = grad_query_terms.astype(jnp.bfloat16)
    grad_keys = lax.psum_scatter(
        grad_kv_terms.astype(jnp.bfloat16), ("expert", "shard"), scatter_dimension=0, tiled=True
    )
    grad_query_slots = send_out(
        matmul(place_attn, grad_queries).astype(jnp.bfloat16).reshape(experts, capacity, qwidth)
    ).reshape(-1, qwidth)
    grad_row_attn = send_back(
        jnp.einsum("rq,dq->rd", grad_query_slots, query_full, preferred_element_type=jnp.float32)
        .astype(jnp.bfloat16)
        .reshape(experts, capacity, D)
    )
    query_grad_term = jnp.einsum(
        "rd,rq->dq", slots_attn, grad_query_slots, preferred_element_type=jnp.float32
    )
    query_grad, output_grad = (
        lax.psum_scatter(
            query_grad_term.astype(jnp.bfloat16), ("dp", "shard"), scatter_dimension=0, tiled=True
        ).astype(jnp.float32),
        lax.psum_scatter(
            output_grad_term.astype(jnp.bfloat16), ("dp", "shard"), scatter_dimension=0, tiled=True
        ).astype(jnp.float32),
    )
    piece = normed_attn
    kv_grad = lax.psum_scatter(
        jnp.einsum("td,tk->dk", piece, grad_keys, preferred_element_type=jnp.float32),
        ("dp", "expert", "shard"),
        scatter_dimension=0,
        tiled=True,
    )
    grad_normed_attn = from_slots(merged_attn, grad_row_attn)
    grad_normed_attn = grad_normed_attn + jnp.einsum(
        "tk,dk->td", grad_keys, kv_full, preferred_element_type=jnp.float32
    )
    router_grad_attn, router_part_attn = router_back(
        gate_attn, grad_gate_attn, chosen_attn, normed_attn, routers[0]
    )
    grad_normed_attn = grad_normed_attn + router_part_attn
    grad_inputs, gain_grad_attn = norm_back(inputs, factor_attn, norm_gains[0], grad_normed_attn)
    grad_inputs = grad_inputs + grad_hidden
    gain_grad, router_grad = lax.psum(
        (
            jnp.stack([gain_grad_attn, gain_grad_mlp]),
            jnp.stack([router_grad_attn, router_grad_mlp]),
        ),
        ("dp", "expert", "shard"),
    )
    return (
        output,
        grad_inputs[None],
        gain_grad,
        router_grad,
        kv_grad,
        query_grad[None],
        output_grad[None],
        inner_grad[None],
        outer_grad[None],
    )


def solution(mesh):
    plane = mesh.shape["expert"] * mesh.shape["shard"]
    fits = HEADS % plane == 0
    return jax.shard_map(
        per_device if fits else per_device_gathered,
        mesh=mesh,
        in_specs=(
            P("dp", ("expert", "shard"), None),
            P(),
            P(),
            P(("dp", "expert", "shard"), None),
            P("expert", ("dp", "shard"), None),
            P("expert", ("dp", "shard"), None),
            P("expert", ("dp", "shard"), None),
            P("expert", ("dp", "shard"), None),
            P("dp", ("expert", "shard"), None),
            P("dp", ("expert", "shard"), None),
            P("dp"),
            P("dp", ("expert", "shard"), None),
        ),
        out_specs=(
            P("dp", ("expert", "shard"), None),
            P("dp", ("expert", "shard"), None),
            P(),
            P(),
            P(("dp", "expert", "shard"), None),
            P("expert", ("dp", "shard"), None),
            P("expert", ("dp", "shard"), None),
            P("expert", ("dp", "shard"), None),
            P("expert", ("dp", "shard"), None),
        ),
        check_vma=False,
    )
```
